32 devices in a mesh: gx: 4 (over z), gy: 4 (over y, x), gz: 2 (over core).
Axes of the slice: x: 2, y: 2, z: 4, core: 2. Of those that a mesh axis runs over, the one named last changes fastest.
Arguments:
- right_side: float32 [4, 96, 96, 48], P(None, 'gx', 'gy', 'gz'), may hold values from -6 to 6
- iterate: float32 [4, 96, 96, 48], P(None, 'gx', 'gy', 'gz'), may hold values from -6 to 6
- coefficient: float32 [96, 96, 48], P('gx', 'gy', 'gz'), may hold values from 0.1 to 2
- ordering: int32 [4, 4, 2, 216], P('gx', 'gy', 'gz'), may hold values from 0 to 215, as said below
- leaf_inverse: float32 [4, 4, 2, 125, 125], P('gx', 'gy', 'gz'), may hold values from -2 to 3
- leaf_first: float32 [4, 4, 2, 125, 50], P('gx', 'gy', 'gz'), may hold values from -0.5 to 0.5
- leaf_second: float32 [4, 4, 2, 125, 60], P('gx', 'gy', 'gz'), may hold values from -0.5 to 0.5
- leaf_top: float32 [4, 4, 2, 125, 72], P('gx', 'gy', 'gz'), may hold values from -0.5 to 0.5
- first_inverse: float32 [4, 4, 50, 50], P('gx', 'gy', 'gz'), may hold values from -2 to 3
- first_second: float32 [4, 4, 2, 25, 60], P('gx', 'gy', 'gz'), may hold values from -1.25 to 1.25
- first_top: float32 [4, 4, 2, 25, 72], P('gx', 'gy', 'gz'), may hold values from -1.25 to 1.25
- second_inverse: float32 [4, 240, 240], P('gx', ('gy', 'gz')), may hold values from -2 to 3
- second_top: float32 [4, 4, 2, 30, 72], P('gx', 'gy', 'gz'), may hold values from -1 to 1
- top_inverse: float32 [1152, 1152], P(('gx', 'gy', 'gz')), may hold values from -2 to 3
Outputs:
- correction: float32 [4, 96, 96, 48], P(None, 'gx', 'gy', 'gz')
The draws below stay inside these ranges and needn't reach their ends.
Inputs may be any that keep to these rules, and one draw needn't show every extreme that they name: `ordering`: each device's row names each of its 216 coarse cells once (cell x 6^2 + y * 6 + z): first the 125 cells with x, y and z all below 5, then the 25 cells with z = 5 and x, y below it, then the 30 cells with y = 5 and x below it, then the 36 cells with x = 5, each group in any order.
All inputs are finite; a program needn't handle non-finite values.
Results may differ from the reference program's by a relative error of at most 0.0003.
Values sent between devices are 32-bit elements; how exact they have to be, the bound alone decides.
A program may use at most 64 MiB of HBM per device.

```python
import math
import jax
import jax.numpy as jnp
from jax import lax

NRHS = 4
SIDE = 6
COARSE_DEV = 216
FIRST_DEV = 25
SECOND_DEV = 30
TOP_DEV = 36
LEAF = 125
FIRST_SEP = 50
SECOND_SEP = 240
TOP_SEP = 1152
NX = 96
NY = 96
NZ = 48
N_GX = 4
N_GY = 4
N_GZ = 2


def inverse_block(key, leading, extent):
    full_shape = tuple(leading) + (extent, extent)
    jitter = jnp.clip(jax.random.normal(key, full_shape, jnp.float32), -4.0, 4.0) * 0.5
    return jnp.eye(extent, dtype=jnp.float32) + jitter / extent ** 0.5


def draw_leaf_inverse(key, part):
    return inverse_block(jax.random.fold_in(key, 11), (N_GX, N_GY, N_GZ), LEAF)


def draw_first_inverse(key, part):
    return inverse_block(jax.random.fold_in(key, 23), (N_GX, N_GY), FIRST_SEP)


def draw_second_inverse(key, part):
    return inverse_block(jax.random.fold_in(key, 37), (N_GX,), SECOND_SEP)


def draw_top_inverse(key, part):
    return inverse_block(jax.random.fold_in(key, 41), (), TOP_SEP)


def draw_ordering(key, part):
    cells = jnp.arange(COARSE_DEV, dtype=jnp.int32)
    first_coord = cells // (SIDE * SIDE)
    second_coord = cells // SIDE % SIDE
    third_coord = cells % SIDE
    edge = SIDE - 1
    classes = jnp.where(first_coord == edge, 3, jnp.where(second_coord == edge, 2, jnp.where(third_coord == edge, 1, 0))).astype(jnp.int32)
    subkeys = jax.random.split(jax.random.fold_in(key, 53), N_GX * N_GY * N_GZ)

    def one_row(subkey):
        shuffled = jax.random.permutation(subkey, COARSE_DEV).astype(jnp.int32)
        rank = jnp.argsort(classes[shuffled], stable=True)
        return shuffled[rank].astype(jnp.int32)
    return jax.vmap(one_row)(subkeys).reshape(N_GX, N_GY, N_GZ, COARSE_DEV)


def levels(own_key, dims, shards, low, top_value):
    factor_of = 1.0
    for axis_at, blocks in shards:
        draws = jax.random.uniform(jax.random.fold_in(jax.random.fold_in(own_key, 6), axis_at), (blocks,), jnp.float32, low / len(shards), top_value / len(shards))
        factor_of = factor_of * jnp.repeat(jnp.exp(draws), dims[axis_at] // blocks).reshape((-1,) + (1,) * (len(dims) - 1 - axis_at))
    return factor_of


def normal_values(stream_key, dims, scale, most, cuts=(), kind=jnp.bfloat16):
    gain = levels(stream_key, dims, cuts, -0.22, 0.18) if cuts else 1.0
    drawn = jax.random.normal(stream_key, dims, jnp.float32) * scale * gain
    return jnp.minimum(jnp.maximum(drawn, -most), most).astype(kind)


def setup_inputs(seed: int = 0) -> dict:
    keys = jax.random.split(jax.random.key(seed), 15)
    return {
        "right_side": normal_values(keys[0], (NRHS, NX, NY, NZ), 1.0, 6.0, ((1, 4), (2, 4), (3, 2)), jnp.float32),
        "iterate": normal_values(keys[1], (NRHS, NX, NY, NZ), 1.0, 6.0, ((1, 4), (2, 4), (3, 2)), jnp.float32),
        "coefficient": jnp.clip(jnp.exp(math.log(2.0) - 2.9957323 * jax.random.uniform(keys[2], (NX, NY, NZ), jnp.float32) ** levels(keys[2], (NX, NY, NZ), ((0, 4), (1, 4), (2, 2)), -0.2, 0.2)), 0.1, 2.0),
        "ordering": draw_ordering(jax.random.fold_in(keys[14], 71), 0),
        "leaf_inverse": draw_leaf_inverse(jax.random.fold_in(keys[14], 71), 0),
        "leaf_first": normal_values(keys[5], (N_GX, N_GY, N_GZ, LEAF, 2 * FIRST_DEV), LEAF ** -0.5, 0.5, ((0, 4), (1, 4), (2, 2)), jnp.float32),
        "leaf_second": normal_values(keys[6], (N_GX, N_GY, N_GZ, LEAF, 2 * SECOND_DEV), LEAF ** -0.5, 0.5, ((0, 4), (1, 4), (2, 2)), jnp.float32),
        "leaf_top": normal_values(keys[7], (N_GX, N_GY, N_GZ, LEAF, 2 * TOP_DEV), LEAF ** -0.5, 0.5, ((0, 4), (1, 4), (2, 2)), jnp.float32),
        "first_inverse": draw_first_inverse(jax.random.fold_in(keys[14], 71), 0),
        "first_second": normal_values(keys[9], (N_GX, N_GY, N_GZ, FIRST_DEV, 2 * SECOND_DEV), FIRST_DEV ** -0.5, 1.25, ((0, 4), (1, 4), (2, 2)), jnp.float32),
        "first_top": normal_values(keys[10], (N_GX, N_GY, N_GZ, FIRST_DEV, 2 * TOP_DEV), FIRST_DEV ** -0.5, 1.25, ((0, 4), (1, 4), (2, 2)), jnp.float32),
        "second_inverse": draw_second_inverse(jax.random.fold_in(keys[14], 71), 0),
        "second_top": normal_values(keys[12], (N_GX, N_GY, N_GZ, SECOND_DEV, 2 * TOP_DEV), SECOND_DEV ** -0.5, 1.0, ((0, 4), (1, 4), (2, 2)), jnp.float32),
        "top_inverse": draw_top_inverse(jax.random.fold_in(keys[14], 71), 0),
    }


precise = lax.Precision.HIGHEST


def contract(pattern, operand, matrix):
    return jnp.einsum(pattern, operand, matrix, precision=precise, preferred_element_type=jnp.float32)


def weigh(extended, dimension):
    length = extended.shape[dimension] - 1
    previous = lax.slice_in_dim(extended, 0, length, 2, dimension)
    centre = lax.slice_in_dim(extended, 1, length + 1, 2, dimension)
    following = lax.slice_in_dim(extended, 2, length + 1, 2, dimension)
    return 0.25 * previous + 0.5 * centre + 0.25 * following


def spread(extended, dimension):
    length = extended.shape[dimension] - 1
    current = lax.slice_in_dim(extended, 0, length, 1, dimension)
    following = lax.slice_in_dim(extended, 1, length + 1, 1, dimension)
    paired = jnp.stack([current, 0.5 * (current + following)], axis=dimension + 1)
    new_shape = list(current.shape)
    new_shape[dimension] = 2 * length
    return paired.reshape(new_shape)


def restrict(values):
    extended = jnp.pad(values, ((0, 0), (1, 0), (1, 0), (1, 0)))
    for dimension in (1, 2, 3):
        extended = weigh(extended, dimension)
    return extended


def prolong(values):
    extended = jnp.pad(values, ((0, 0), (0, 1), (0, 1), (0, 1)))
    for dimension in (1, 2, 3):
        extended = spread(extended, dimension)
    return extended


def residual_of(right_side, iterate, coefficient):
    padded = jnp.pad(iterate, ((0, 0), (1, 1), (1, 1), (1, 1)))
    beside = padded[:, 2:, 1:-1, 1:-1] + padded[:, :-2, 1:-1, 1:-1]
    beside = beside + padded[:, 1:-1, 2:, 1:-1] + padded[:, 1:-1, :-2, 1:-1]
    beside = beside + padded[:, 1:-1, 1:-1, 2:] + padded[:, 1:-1, 1:-1, :-2]
    return right_side - ((6.0 + coefficient) * iterate - beside)


def from_above(values, axis):
    length = values.shape[axis]
    kept = lax.slice_in_dim(values, 1, length, 1, axis)
    widths = [(0, 0)] * values.ndim
    widths[axis] = (0, 1)
    return jnp.pad(kept, widths)


def from_below(values, axis):
    length = values.shape[axis]
    kept = lax.slice_in_dim(values, 0, length - 1, 1, axis)
    widths = [(0, 0)] * values.ndim
    widths[axis] = (1, 0)
    return jnp.pad(kept, widths)


def reference(right_side, iterate, coefficient, ordering, leaf_inverse, leaf_first, leaf_second, leaf_top, first_inverse, first_second, first_top, second_inverse, second_top, top_inverse):
    coarse = restrict(restrict(residual_of(right_side, iterate, coefficient)))
    blocks = coarse.reshape(NRHS, N_GX, SIDE, N_GY, SIDE, N_GZ, SIDE)
    blocks = blocks.transpose(0, 1, 3, 5, 2, 4, 6).reshape(NRHS, N_GX, N_GY, N_GZ, COARSE_DEV)
    chosen = jnp.take_along_axis(blocks, jnp.broadcast_to(ordering[None], blocks.shape), axis=4)
    first_end = LEAF + FIRST_DEV
    second_end = first_end + SECOND_DEV
    leaf_rhs = chosen[..., :LEAF]
    first_rhs = chosen[..., LEAF:first_end]
    second_rhs = chosen[..., first_end:second_end]
    top_rhs = chosen[..., second_end:]

    leaf_solved = contract('rabcl,abclk->rabck', leaf_rhs, leaf_inverse)
    toward = contract('rabcl,abclk->rabck', leaf_solved, leaf_first)
    first_target = first_rhs - toward[..., :FIRST_DEV] - from_above(toward[..., FIRST_DEV:], 3)
    first_target = first_target.reshape(NRHS, N_GX, N_GY, FIRST_SEP)
    first_solved = contract('rabi,abik->rabk', first_target, first_inverse).reshape(NRHS, N_GX, N_GY, N_GZ, FIRST_DEV)

    toward = contract('rabcl,abclk->rabck', leaf_solved, leaf_second) + contract('rabcl,abclk->rabck', first_solved, first_second)
    second_target = second_rhs - toward[..., :SECOND_DEV] - from_above(toward[..., SECOND_DEV:], 2)
    second_target = second_target.reshape(NRHS, N_GX, SECOND_SEP)
    second_solved = contract('rai,aik->rak', second_target, second_inverse).reshape(NRHS, N_GX, N_GY, N_GZ, SECOND_DEV)

    toward = contract('rabcl,abclk->rabck', leaf_solved, leaf_top) + contract('rabcl,abclk->rabck', first_solved, first_top)
    toward = toward + contract('rabcl,abclk->rabck', second_solved, second_top)
    top_target = top_rhs - toward[..., :TOP_DEV] - from_above(toward[..., TOP_DEV:], 1)
    top_target = top_target.reshape(NRHS, TOP_SEP)
    top_solved = contract('ri,ik->rk', top_target, top_inverse)

    top_back = contract('rk,ik->ri', top_solved, top_inverse).reshape(NRHS, N_GX, N_GY, N_GZ, TOP_DEV)
    top_pair = jnp.concatenate([top_back, from_below(top_back, 1)], axis=4)
    second_gap = second_solved - contract('rabck,abcik->rabci', top_pair, second_top)
    second_gap = second_gap.reshape(NRHS, N_GX, SECOND_SEP)
    second_back = contract('rak,aik->rai', second_gap, second_inverse).reshape(NRHS, N_GX, N_GY, N_GZ, SECOND_DEV)
    second_pair = jnp.concatenate([second_back, from_below(second_back, 2)], axis=4)
    first_gap = first_solved - contract('rabck,abcik->rabci', second_pair, first_second)
    first_gap = first_gap - contract('rabck,abcik->rabci', top_pair, first_top)
    first_gap = first_gap.reshape(NRHS, N_GX, N_GY, FIRST_SEP)
    first_back = contract('rabk,abik->rabi', first_gap, first_inverse).reshape(NRHS, N_GX, N_GY, N_GZ, FIRST_DEV)
    first_pair = jnp.concatenate([first_back, from_below(first_back, 3)], axis=4)
    leaf_gap = leaf_solved - contract('rabck,abcik->rabci', first_pair, leaf_first)
    leaf_gap = leaf_gap - contract('rabck,abcik->rabci', second_pair, leaf_second)
    leaf_gap = leaf_gap - contract('rabck,abcik->rabci', top_pair, leaf_top)
    leaf_back = contract('rabck,abclk->rabcl', leaf_gap, leaf_inverse)

    ordered = jnp.concatenate([leaf_back, first_back, second_back, top_back], axis=4)
    inverse_order = jnp.argsort(ordering, axis=-1).astype(jnp.int32)
    listed = jnp.take_along_axis(ordered, jnp.broadcast_to(inverse_order[None], ordered.shape), axis=4)
    listed = listed.reshape(NRHS, N_GX, N_GY, N_GZ, SIDE, SIDE, SIDE)
    coarse_grid = listed.transpose(0, 1, 4, 2, 5, 3, 6).reshape(NRHS, N_GX * SIDE, N_GY * SIDE, N_GZ * SIDE)
    return prolong(prolong(coarse_grid))
```

```python
import functools

import jax
import jax.numpy as jnp
import numpy as np
from jax import lax
from jax.experimental import pallas as pl
from jax.experimental.pallas import tpu as pltpu
from jax.sharding import PartitionSpec as P

AXES = ("gx", "gy", "gz")
LANES = 128
SIDES = (0, 1, -1)
MESH = pl.DeviceIdType.MESH
f32 = jnp.float32

SHARES = [
    (i, j, k)
    for i in SIDES
    for j in SIDES
    for k in SIDES
    if (i, j, k) != (0, 0, 0) and (i, j, k).count(-1) <= 1
]
RIMS = [(i, j, k) for i in (0, 1) for j in (0, 1) for k in (0, 1) if (i, j, k) != (0, 0, 0)]


def weight(k):
    return max(0, 4 - abs(k)) / 16.0


def weight_beside(k):
    return weight(k - 1) + weight(k + 1)


def dot(a, b):
    return jnp.dot(a, b, precision=lax.Precision.HIGHEST, preferred_element_type=f32)


def dot_back(a, b):
    return lax.dot_general(
        a, b, (((1,), (1,)), ((), ())),
        precision=lax.Precision.HIGHEST, preferred_element_type=f32,
    )


def coarse_at(side, row, count):
    if side == 0:
        return row if row < count else None
    if side == 1:
        return count if row == 0 else None
    return -1 if row == count - 1 else None


def restriction(fine, pad, stencil):
    count = fine // 4
    out = np.zeros((3, pad, fine), np.float32)
    for s, side in enumerate(SIDES):
        for row in range(pad):
            at = coarse_at(side, row, count)
            if at is not None:
                for y in range(fine):
                    out[s, row, y] = stencil(y - 4 * at)
    return out


def at_first(table):
    table = table.copy()
    table[0, 0, 0] -= weight(-1)
    return table


def interpolation(fine, pad):
    count = fine // 4
    out = np.zeros((2, fine, pad), np.float32)
    for y in range(fine):
        for at in (y // 4, y // 4 + 1):
            value = 1.0 - abs(y - 4 * at) / 4.0
            if at < count:
                out[0, y, at] = value
            else:
                out[1, y, 0] = value
    return out


def constants(rhs, ny, nz, slabs, pad_y, pad_z, rims):
    plain = restriction(ny, pad_y, weight)
    beside = restriction(ny, pad_y, weight_beside)
    eye = np.eye(slabs, dtype=np.float32)
    rows = np.stack([
        np.concatenate(
            [np.concatenate([np.kron(eye, plain[s]), np.kron(eye, b[s])], 1) for s in range(3)], 0
        )
        for b in (at_first(beside), beside)
    ])

    def over_lanes(table):
        out = np.zeros((3, rhs * nz, LANES), np.float32)
        for s in range(3):
            for r in range(rhs):
                out[s, r * nz:(r + 1) * nz, r * pad_z:(r + 1) * pad_z] = table[s].T
        return np.concatenate(list(out), 1)

    lanes = over_lanes(restriction(nz, pad_z, weight))
    table = restriction(nz, pad_z, weight_beside)
    lanes_beside = np.stack([over_lanes(at_first(table)), over_lanes(table)])
    grow = interpolation(nz, pad_z)
    wide = np.zeros((2, LANES, rhs * nz), np.float32)
    for s in range(2):
        for r in range(rhs):
            wide[s, r * pad_z:(r + 1) * pad_z, r * nz:(r + 1) * nz] = grow[s].T
    eye = np.eye(rims, dtype=np.float32)
    tall_of = interpolation(ny, pad_y)
    tall = np.stack([np.kron(eye, tall_of[s]) for s in range(2)])
    return rows, lanes, lanes_beside, wide, tall


def kernel(
    sizes,
    right_ref, u_ref, coef_ref, order_ref, leaf_ref, leaf_links, links_fs, links_ft, links_st,
    rows_first, rows_second, rows_top,
    mat_rows, mat_lanes, mat_beside, mat_wide, mat_tall,
    out_ref,
    packed, shares, total, share_in, prev, scatter_out, scatter_in, gather_in, whole, pairs,
    picked, ordered, rim, stage,
    share_send, share_recv, prev_send, prev_recv, s_send, s_recv, g_send, g_recv, r_send, r_recv,
):
    rhs, nx, ny, nz = u_ref.shape
    side = nx // 4
    side_y, side_z = ny // 4, nz // 4
    slabs = side + 2
    pad_y, pad_z = sizes["pad_y"], sizes["pad_z"]
    me = {a: lax.axis_index(a) for a in AXES}
    peers = sizes["peers"]
    rows_refs = (rows_first, rows_second, rows_top)
    groups = (("gz",), ("gy", "gz"), AXES)
    shift_axis = ("gz", "gy", "gx")
    counts = [int(np.prod([peers[a] for a in g])) for g in groups]

    def place(group):
        at = 0
        for a in group:
            at = at * peers[a] + me[a]
        return at

    def coords(group, at):
        found = {}
        for a in reversed(group):
            found[a] = at % peers[a]
            at = at // peers[a]
        return {a: found[a] if a in found else me[a] for a in AXES}

    prev_copies = []
    for level in range(3):
        axis = shift_axis[level]
        target = dict(me)
        target[axis] = (me[axis] + 1) % peers[axis]
        copy = pltpu.make_async_remote_copy(
            src_ref=rows_refs[level], dst_ref=prev[level],
            send_sem=prev_send.at[level], recv_sem=prev_recv.at[level],
            device_id=target, device_id_type=MESH,
        )
        prev_copies.append(copy)

        @pl.when(me[axis] < peers[axis] - 1)
        def _():
            copy.start()

        @pl.when(me[axis] == 0)
        def _():
            prev[level][...] = jnp.zeros(prev[level].shape, f32)

    half = slabs * ny
    for r in range(rhs):
        acc_p = {}
        acc_u = {}

        def add(acc, at, factor, value):
            term = factor * value
            acc[at] = acc[at] + term if at in acc else term

        for x in range(nx):
            u = u_ref[r, x]
            q = right_ref[r, x] - (6.0 + coef_ref[x]) * u
            for at in range(-1, side + 1):
                k = x - 4 * at
                if weight(k):
                    add(acc_p, at, weight(k), q)
                    add(acc_u, at, weight(k), u)
                if at == 0 and x == 0:
                    below = jnp.where(me["gx"] > 0, weight(-1), 0.0)
                    add(acc_p, at, weight(1) + below, u)
                elif weight_beside(k):
                    add(acc_p, at, weight_beside(k), u)
        for at in range(-1, side + 1):
            rows = slice((at + 1) * ny, (at + 2) * ny)
            packed[rows, r * nz:(r + 1) * nz] = acc_p[at]
            rows = slice(half + (at + 1) * ny, half + (at + 2) * ny)
            packed[rows, r * nz:(r + 1) * nz] = acc_u.get(at, jnp.zeros((ny, nz), f32))
    both = packed[...]
    at_y, at_z = jnp.minimum(me["gy"], 1), jnp.minimum(me["gz"], 1)
    a = dot(mat_rows[at_y], both)
    b = dot(mat_rows[1, :, :half], both[half:])
    c = dot(a, mat_lanes[...]) + dot(b, mat_beside[at_z])
    for s in range(3):
        for t in range(3):
            part = c[s * slabs * pad_y:(s + 1) * slabs * pad_y, t * LANES:(t + 1) * LANES]
            shares[s, t] = part.reshape(slabs, pad_y, LANES)

    def valid(step, sign):
        ok = None
        for a, d in zip(AXES, step):
            if d:
                at = me[a] + sign * d
                this = (at >= 0) & (at < peers[a])
                ok = this if ok is None else ok & this
        return ok

    def toward(step, sign):
        return {a: (me[a] + sign * d + peers[a]) % peers[a] for a, d in zip(AXES, step)}

    share_copies = []
    for n, step in enumerate(SHARES):
        dx, dy, dz = step
        cut = {0: pl.ds(1, side), 1: pl.ds(side + 1, 1), -1: pl.ds(0, 1)}[dx]
        copy = pltpu.make_async_remote_copy(
            src_ref=shares.at[SIDES.index(dy), SIDES.index(dz), cut],
            dst_ref=share_in[n],
            send_sem=share_send.at[n], recv_sem=share_recv.at[n],
            device_id=toward(step, 1), device_id_type=MESH,
        )
        share_copies.append(copy)

        @pl.when(valid(step, 1))
        def _():
            copy.start()

    total[...] = shares[0, 0, 1:side + 1]

    order = order_ref[...].astype(f32)
    first = jnp.floor((order + 0.5) / (side_y * side_z))
    rest = order - first * (side_y * side_z)
    second = jnp.floor((rest + 0.5) / side_z)
    third = rest - second * side_z
    cells = order.shape[1]
    spots = side * pad_y
    row_id = lax.broadcasted_iota(jnp.int32, (spots, cells), 0).astype(f32)
    row_hot = (row_id == first * pad_y + second).astype(f32)
    lane_id = lax.broadcasted_iota(jnp.int32, (LANES, cells), 0).astype(f32)

    def lane_hot(r):
        return (lane_id == third + r * pad_z).astype(f32)

    for n, step in enumerate(SHARES):
        @pl.when(valid(step, -1))
        def _():
            share_copies[n].wait_recv()
            if step[0] == 0:
                total[...] += share_in[n][...]
            elif step[0] == 1:
                total[0] += share_in[n][0]
            else:
                total[side - 1] += share_in[n][0]

    coarse = total[...].reshape(spots, LANES)
    for r in range(rhs):
        spread = dot(coarse, lane_hot(r))
        picked[r:r + 1, :] = jnp.sum(spread * row_hot, axis=0, keepdims=True)

    leaf = leaf_ref.shape[0]
    spans = [rows.shape[0] for rows in rows_refs]
    starts = [leaf, leaf + spans[0], leaf + spans[0] + spans[1]]
    leaf_solved = dot(picked[:, :leaf], leaf_ref[...])

    def all_slots(buffer, sem, count):
        return pltpu.make_async_copy(
            buffer.at[pl.ds(0, count - 1)], buffer.at[pl.ds(0, count - 1)], sem
        )

    def forward(level, toward_low):
        span, count, group = spans[level], counts[level], groups[level]
        axis = shift_axis[level]
        target = picked[:, starts[level]:starts[level] + span] - toward_low[:, :span]

        @pl.when(me[axis] > 0)
        def _():
            prev_copies[level].wait_recv()

        terms = dot(target, rows_refs[level][...]) - dot(toward_low[:, span:], prev[level][...])
        out, into = scatter_out[level], scatter_in[level]
        for d in range(count):
            out[d, :, :span] = terms[:, d * span:(d + 1) * span]
        mine = place(group)

        def send(k, carry):
            d = (mine + k) % count
            pltpu.make_async_remote_copy(
                src_ref=out.at[d], dst_ref=into.at[mine],
                send_sem=s_send.at[level], recv_sem=s_recv.at[level],
                device_id=coords(group, d), device_id_type=MESH,
            ).start()
            return carry

        lax.fori_loop(1, count, send, 0)
        into[mine] = out[mine]
        all_slots(into, s_recv.at[level], count).wait()
        return jnp.sum(into[...], axis=0)[:, :span]

    def backward(level, gap):
        span, count, group = spans[level], counts[level], groups[level]
        into = gather_in[level]
        own = stage[level]
        mine = place(group)
        own[:, :span] = gap

        def send(k, carry):
            d = (mine + k) % count
            pltpu.make_async_remote_copy(
                src_ref=own, dst_ref=into.at[mine],
                send_sem=g_send.at[level], recv_sem=g_recv.at[level],
                device_id=coords(group, d), device_id_type=MESH,
            ).start()
            return carry

        lax.fori_loop(1, count, send, 0)
        into[mine] = own[...]
        all_slots(into, g_recv.at[level], count).wait()
        full = whole[level]
        for d in range(count):
            full[:, d * span:(d + 1) * span] = into[d, :, :span]
        value = full[...]
        pair = pairs[level]
        back = dot_back(value, rows_refs[level][...])
        pair[:, :span] = back
        pair[:, span:] = dot_back(value, prev[level][...])
        return back, pair[...]

    to_first, to_second, to_top = (link[...] for link in leaf_links)
    first_own = forward(0, dot(leaf_solved, to_first))
    second_own = forward(1, dot(leaf_solved, to_second) + dot(first_own, links_fs[...]))
    top_own = forward(
        2,
        dot(leaf_solved, to_top) + dot(first_own, links_ft[...]) + dot(second_own, links_st[...]),
    )
    top_back, top_pair = backward(2, top_own)
    second_back, second_pair = backward(1, second_own - dot_back(top_pair, links_st[...]))
    first_back, first_pair = backward(
        0,
        first_own - dot_back(second_pair, links_fs[...]) - dot_back(top_pair, links_ft[...]),
    )
    leaf_gap = leaf_solved - dot_back(first_pair, to_first) - dot_back(second_pair, to_second)
    leaf_back = dot_back(leaf_gap - dot_back(top_pair, to_top), leaf_ref[...])
    ordered[:, :leaf] = leaf_back
    ordered[:, starts[0]:starts[1]] = first_back
    ordered[:, starts[1]:starts[2]] = second_back
    ordered[:, starts[2]:] = top_back

    cells_back = None
    for r in range(rhs):
        term = dot_back(row_hot * ordered[r:r + 1, :], lane_hot(r))
        cells_back = term if cells_back is None else cells_back + term
    rim[0, 0, 0:side] = cells_back.reshape(side, pad_y, LANES)

    rim_copies = []
    for n, step in enumerate(RIMS):
        dx, dy, dz = step
        source = rim.at[0, 0, pl.ds(0, 1 if dx else side)]
        landing = rim.at[dy, dz, pl.ds(side, 1) if dx else pl.ds(0, side)]
        copy = pltpu.make_async_remote_copy(
            src_ref=source, dst_ref=landing,
            send_sem=r_send.at[n], recv_sem=r_recv.at[n],
            device_id=toward(step, -1), device_id_type=MESH,
        )
        rim_copies.append(copy)

        @pl.when(valid(step, -1))
        def _():
            copy.start()

    for n, step in enumerate(RIMS):
        dx, dy, dz = step
        here = valid(step, 1)

        @pl.when(here)
        def _():
            rim_copies[n].wait_recv()

        @pl.when(jnp.logical_not(here))
        def _():
            if dx:
                rim[dy, dz, side] = jnp.zeros((pad_y, LANES), f32)
            else:
                rim[dy, dz, 0:side] = jnp.zeros((side, pad_y, LANES), f32)

    tall_rows = (side + 1) * pad_y
    grown = None
    for s in range(2):
        wide = dot(rim[s, 0].reshape(tall_rows, LANES), mat_wide[0])
        wide = wide + dot(rim[s, 1].reshape(tall_rows, LANES), mat_wide[1])
        term = dot(mat_tall[s], wide)
        grown = term if grown is None else grown + term
    for r in range(rhs):
        slices = [
            grown[at * ny:(at + 1) * ny, r * nz:(r + 1) * nz] for at in range(side + 1)
        ]
        for x in range(nx):
            at, k = x // 4, x % 4
            if k == 0:
                out_ref[r, x] = slices[at]
            else:
                out_ref[r, x] = (1 - k / 4) * slices[at] + (k / 4) * slices[at + 1]

    for level in range(3):
        axis = shift_axis[level]

        @pl.when(me[axis] < peers[axis] - 1)
        def _():
            prev_copies[level].wait_send()

        all_slots(scatter_out[level], s_send.at[level], counts[level]).wait()
        all_slots(gather_in[level], g_send.at[level], counts[level]).wait()
    for n, step in enumerate(SHARES):
        @pl.when(valid(step, 1))
        def _():
            share_copies[n].wait_send()
    for n, step in enumerate(RIMS):
        @pl.when(valid(step, -1))
        def _():
            rim_copies[n].wait_send()


def per_device(peers, right_side, iterate, coefficient, ordering, leaf_inverse, leaf_first,
               leaf_second, leaf_top, first_inverse, first_second, first_top, second_inverse,
               second_top, top_inverse):
    rhs, nx, ny, nz = iterate.shape
    side = nx // 4
    slabs = side + 2
    pad_y = -(-(ny // 4) // 8) * 8
    pad_z = LANES // rhs // 4 if nz // 4 <= LANES // rhs // 4 else LANES // rhs
    mats = constants(rhs, ny, nz, slabs, pad_y, pad_z, side + 1)
    flat = lambda m: m.reshape(m.shape[-2:])
    rows = [flat(first_inverse), flat(second_inverse), top_inverse]
    spans = [m.shape[0] for m in rows]
    counts = [m.shape[1] // m.shape[0] for m in rows]
    cells = ordering.shape[-1]
    vmem = lambda *shape: pltpu.VMEM(shape, f32)
    dma = lambda n: pltpu.SemaphoreType.DMA((n,))
    tile = (pad_y, LANES)
    sizes = {"peers": peers, "pad_y": pad_y, "pad_z": pad_z}
    operands = (
        right_side, iterate, coefficient, ordering.reshape(1, cells), flat(leaf_inverse),
        (flat(leaf_first), flat(leaf_second), flat(leaf_top)),
        flat(first_second), flat(first_top), flat(second_top), *rows,
        *[jnp.asarray(m) for m in mats],
    )
    in_vmem = pl.BlockSpec(memory_space=pltpu.VMEM)
    return pl.pallas_call(
        functools.partial(kernel, sizes),
        out_shape=jax.ShapeDtypeStruct(iterate.shape, f32),
        in_specs=jax.tree.map(lambda _: in_vmem, operands),
        out_specs=in_vmem,
        scratch_shapes=[
            vmem(2 * slabs * ny, rhs * nz),
            vmem(3, 3, slabs, *tile),
            vmem(side, *tile),
            [vmem(side if step[0] == 0 else 1, *tile) for step in SHARES],
            [vmem(*m.shape) for m in rows],
            [vmem(n, rhs, LANES) for n in counts],
            [vmem(n, rhs, LANES) for n in counts],
            [vmem(n, rhs, LANES) for n in counts],
            [vmem(rhs, m.shape[1]) for m in rows],
            [vmem(rhs, 2 * s) for s in spans],
            vmem(rhs, cells),
            vmem(rhs, cells),
            vmem(2, 2, side + 1, *tile),
            [vmem(rhs, LANES) for _ in rows],
            dma(len(SHARES)), dma(len(SHARES)), dma(3), dma(3), dma(3), dma(3), dma(3), dma(3),
            dma(len(RIMS)), dma(len(RIMS)),
        ],
        compiler_params=pltpu.CompilerParams(has_side_effects=True),
    )(*operands)


def solution(mesh):
    peers = dict(mesh.shape)
    return jax.shard_map(
        functools.partial(per_device, peers),
        mesh=mesh,
        in_specs=(
            P(None, "gx", "gy", "gz"),
            P(None, "gx", "gy", "gz"),
            P("gx", "gy", "gz"),
            P("gx", "gy", "gz", None),
            P("gx", "gy", "gz", None, None),
            P("gx", "gy", "gz", None, None),
            P("gx", "gy", "gz", None, None),
            P("gx", "gy", "gz", None, None),
            P("gx", "gy", "gz", None),
            P("gx", "gy", "gz", None, None),
            P("gx", "gy", "gz", None, None),
            P("gx", ("gy", "gz"), None),
            P("gx", "gy", "gz", None, None),
            P(("gx", "gy", "gz"), None),
        ),
        out_specs=P(None, "gx", "gy", "gz"),
        check_vma=False,
    )
```

```python
import functools

import jax
import jax.numpy as jnp
import numpy as np
from jax import lax
from jax.experimental import pallas as pl
from jax.experimental.pallas import tpu as pltpu
from jax.sharding import PartitionSpec as P

AXES = ("gx", "gy", "gz")
LANES = 128
SIDES = (0, 1, -1)
MESH = pl.DeviceIdType.MESH
f32 = jnp.float32
bf16 = jnp.bfloat16

SHARES = [
    (i, j, k)
    for i in SIDES
    for j in SIDES
    for k in SIDES
    if (i, j, k) != (0, 0, 0) and (i, j, k).count(-1) <= 1
]
RIMS = [(i, j, k) for i in (0, 1) for j in (0, 1) for k in (0, 1) if (i, j, k) != (0, 0, 0)]


def weight(k):
    return max(0, 4 - abs(k)) / 16.0


def weight_beside(k):
    return weight(k - 1) + weight(k + 1)


def single(a, b):
    return jnp.dot(a, b, preferred_element_type=f32)


def single_back(a, b):
    return lax.dot_general(a, b, (((1,), (1,)), ((), ())), preferred_element_type=f32)


def halves(x):
    high = x.astype(bf16)
    return high, (x - high.astype(f32)).astype(bf16)


def stacked(x):
    high = x.astype(bf16).astype(f32)
    return jnp.concatenate([high, x - high], axis=0).astype(bf16)


def dot_exact(a, b, product=single):
    high, low = halves(a)
    return product(high, b) + product(low, b)


def dot(a, b, product=single):
    count = a.shape[0]
    both = product(stacked(a), b[0][...])
    return both[:count] + both[count:] + product(a.astype(bf16), b[1][...])


def dot_back(a, b):
    return dot(a, b, single_back)


def coarse_at(side, row, count):
    if side == 0:
        return row if row < count else None
    if side == 1:
        return count if row == 0 else None
    return -1 if row == count - 1 else None


def restriction(fine, pad, stencil):
    count = fine // 4
    out = np.zeros((3, pad, fine), np.float32)
    for s, side in enumerate(SIDES):
        for row in range(pad):
            at = coarse_at(side, row, count)
            if at is not None:
                for y in range(fine):
                    out[s, row, y] = stencil(y - 4 * at)
    return out


def at_first(table):
    table = table.copy()
    table[0, 0, 0] -= weight(-1)
    return table


def interpolation(fine, pad):
    count = fine // 4
    out = np.zeros((2, fine, pad), np.float32)
    for y in range(fine):
        for at in (y // 4, y // 4 + 1):
            value = 1.0 - abs(y - 4 * at) / 4.0
            if at < count:
                out[0, y, at] = value
            else:
                out[1, y, 0] = value
    return out


def constants(rhs, ny, nz, slabs, pad_y, pad_z, rims):
    plain = restriction(ny, pad_y, weight)
    beside = restriction(ny, pad_y, weight_beside)
    eye = np.eye(slabs, dtype=np.float32)
    rows = np.stack([
        np.concatenate(
            [np.concatenate([np.kron(eye, plain[s]), np.kron(eye, b[s])], 1) for s in range(3)], 0
        )
        for b in (at_first(beside), beside)
    ])

    def over_lanes(table):
        out = np.zeros((3, rhs * nz, LANES), np.float32)
        for s in range(3):
            for r in range(rhs):
                out[s, r * nz:(r + 1) * nz, r * pad_z:(r + 1) * pad_z] = table[s].T
        return np.concatenate(list(out), 1)

    lanes = over_lanes(restriction(nz, pad_z, weight))
    table = restriction(nz, pad_z, weight_beside)
    lanes_beside = np.stack([over_lanes(at_first(table)), over_lanes(table)])
    grow = interpolation(nz, pad_z)
    wide = np.zeros((2, LANES, rhs * nz), np.float32)
    for s in range(2):
        for r in range(rhs):
            wide[s, r * pad_z:(r + 1) * pad_z, r * nz:(r + 1) * nz] = grow[s].T
    eye = np.eye(rims, dtype=np.float32)
    tall_of = interpolation(ny, pad_y)
    tall = np.stack([np.kron(eye, tall_of[s]) for s in range(2)])
    return rows, lanes, lanes_beside, wide, tall


def kernel(
    sizes,
    right_ref, u_ref, coef_ref, order_ref, leaf_raw, leaf_first_raw, leaf_second_raw,
    leaf_top_ref, fs_raw, ft_raw, st_raw, rows_first, rows_second, rows_top,
    mat_rows, mat_lanes, mat_beside, mat_wide, mat_tall,
    out_ref,
    split_leaf, split_links, split_fs, split_ft, split_st, split_rows, left,
    packed, shares, total, share_in, prev, scatter_out, scatter_in, gather_in, whole, pairs,
    picked, ordered, rim, stage,
    share_send, share_recv, prev_send, prev_recv, s_send, s_recv, g_send, g_recv, r_send, r_recv,
):
    rhs, nx, ny, nz = u_ref.shape
    side = nx // 4
    side_y, side_z = ny // 4, nz // 4
    slabs = side + 2
    pad_y, pad_z = sizes["pad_y"], sizes["pad_z"]
    me = {a: lax.axis_index(a) for a in AXES}
    peers = sizes["peers"]
    rows_refs = (rows_first, rows_second, rows_top)
    groups = (("gz",), ("gy", "gz"), AXES)
    shift_axis = ("gz", "gy", "gx")
    counts = [int(np.prod([peers[a] for a in g])) for g in groups]

    def place(group):
        at = 0
        for a in group:
            at = at * peers[a] + me[a]
        return at

    def coords(group, at):
        found = {}
        for a in reversed(group):
            found[a] = at % peers[a]
            at = at // peers[a]
        return {a: found[a] if a in found else me[a] for a in AXES}

    prev_copies = []
    for level in range(3):
        axis = shift_axis[level]
        target = dict(me)
        target[axis] = (me[axis] + 1) % peers[axis]
        copy = pltpu.make_async_remote_copy(
            src_ref=rows_refs[level], dst_ref=prev[level],
            send_sem=prev_send.at[level], recv_sem=prev_recv.at[level],
            device_id=target, device_id_type=MESH,
        )
        prev_copies.append(copy)

        @pl.when(me[axis] < peers[axis] - 1)
        def _():
            if level < 2:
                copy.start()

        @pl.when(me[axis] == 0)
        def _():
            prev[level][...] = jnp.zeros(prev[level].shape, f32)

    half = slabs * ny
    for r in range(rhs):
        acc_p = {}
        acc_u = {}

        def add(acc, at, factor, value):
            term = factor * value
            acc[at] = acc[at] + term if at in acc else term

        for x in range(nx):
            u = u_ref[r, x]
            q = right_ref[r, x] - (6.0 + coef_ref[x]) * u
            for at in range(-1, side + 1):
                k = x - 4 * at
                if weight(k):
                    add(acc_p, at, weight(k), q)
                    add(acc_u, at, weight(k), u)
                if at == 0 and x == 0:
                    below = jnp.where(me["gx"] > 0, weight(-1), 0.0)
                    add(acc_p, at, weight(1) + below, u)
                elif weight_beside(k):
                    add(acc_p, at, weight_beside(k), u)
        for at in range(-1, side + 1):
            rows = slice((at + 1) * ny, (at + 2) * ny)
            packed[rows, r * nz:(r + 1) * nz] = acc_p[at]
            rows = slice(half + (at + 1) * ny, half + (at + 2) * ny)
            packed[rows, r * nz:(r + 1) * nz] = acc_u.get(at, jnp.zeros((ny, nz), f32))
    both = packed[...]
    at_y, at_z = jnp.minimum(me["gy"], 1), jnp.minimum(me["gz"], 1)
    high, low = halves(both)
    a = single(mat_rows[at_y], high) + single(mat_rows[at_y], low)
    b = single(mat_rows[1, :, :half], high[half:]) + single(mat_rows[1, :, :half], low[half:])
    c = dot_exact(a, mat_lanes[...]) + dot_exact(b, mat_beside[at_z])
    for s in range(3):
        for t in range(3):
            part = c[s * slabs * pad_y:(s + 1) * slabs * pad_y, t * LANES:(t + 1) * LANES]
            shares[s, t] = part.reshape(slabs, pad_y, LANES)

    def valid(step, sign):
        ok = None
        for a, d in zip(AXES, step):
            if d:
                at = me[a] + sign * d
                this = (at >= 0) & (at < peers[a])
                ok = this if ok is None else ok & this
        return ok

    def toward(step, sign):
        return {a: (me[a] + sign * d + peers[a]) % peers[a] for a, d in zip(AXES, step)}

    share_copies = []
    for n, step in enumerate(SHARES):
        dx, dy, dz = step
        cut = {0: pl.ds(1, side), 1: pl.ds(side + 1, 1), -1: pl.ds(0, 1)}[dx]
        copy = pltpu.make_async_remote_copy(
            src_ref=shares.at[SIDES.index(dy), SIDES.index(dz), cut],
            dst_ref=share_in[n],
            send_sem=share_send.at[n], recv_sem=share_recv.at[n],
            device_id=toward(step, 1), device_id_type=MESH,
        )
        share_copies.append(copy)

        @pl.when(valid(step, 1))
        def _():
            copy.start()

    @pl.when(me[shift_axis[2]] < peers[shift_axis[2]] - 1)
    def _():
        prev_copies[2].start()

    total[...] = shares[0, 0, 1:side + 1]

    def keep(where, value):
        where[0][...], where[1][...] = halves(value)

    def rows_of(raw):
        return raw[:, 0, :] if len(raw.shape) == 3 else raw[...]

    spans = [rows.shape[0] for rows in rows_refs]
    seats = [split_rows[level][0].shape[0] // 2 for level in range(3)]

    def keep_rows(level, at, value):
        high, low = halves(value)
        split_rows[level][0][at:at + spans[level], :] = high
        split_rows[level][1][at:at + spans[level], :] = low

    keep(split_leaf, rows_of(leaf_raw))
    for where, raw in zip(split_links, (leaf_first_raw, leaf_second_raw, leaf_top_ref)):
        keep(where, rows_of(raw))
    keep(split_fs, rows_of(fs_raw))
    keep(split_ft, rows_of(ft_raw))
    keep(split_st, rows_of(st_raw))
    for level in range(3):
        for part in split_rows[level]:
            part[...] = jnp.zeros(part.shape, bf16)
        left[level][...] = jnp.zeros(left[level].shape, f32)
        keep_rows(level, 0, rows_of(rows_refs[level]))

    def settle(level):
        axis = shift_axis[level]

        @pl.when(me[axis] > 0)
        def _():
            prev_copies[level].wait_recv()

        keep_rows(level, seats[level], rows_of(prev[level]))

    settle(0)
    settle(1)

    order = order_ref[...].astype(f32)
    first = jnp.floor((order + 0.5) / (side_y * side_z))
    rest = order - first * (side_y * side_z)
    second = jnp.floor((rest + 0.5) / side_z)
    third = rest - second * side_z
    cells = order.shape[1]
    spots = side * pad_y
    row_id = lax.broadcasted_iota(jnp.int32, (spots, cells), 0).astype(f32)
    row_hot = (row_id == first * pad_y + second).astype(f32)
    lane_id = lax.broadcasted_iota(jnp.int32, (LANES, cells), 0).astype(f32)

    def lane_hot(r):
        return (lane_id == third + r * pad_z).astype(f32).astype(bf16)

    for n, step in enumerate(SHARES):
        @pl.when(valid(step, -1))
        def _():
            share_copies[n].wait_recv()
            if step[0] == 0:
                total[...] += share_in[n][...]
            elif step[0] == 1:
                total[0] += share_in[n][0]
            else:
                total[side - 1] += share_in[n][0]

    coarse = total[...].reshape(spots, LANES)
    for r in range(rhs):
        spread = dot_exact(coarse, lane_hot(r))
        picked[r:r + 1, :] = jnp.sum(spread * row_hot, axis=0, keepdims=True)

    leaf = leaf_raw.shape[0]
    starts = [leaf, leaf + spans[0], leaf + spans[0] + spans[1]]
    leaf_solved = dot(picked[:, :leaf], split_leaf)

    def all_slots(buffer, sem, count):
        return pltpu.make_async_copy(
            buffer.at[pl.ds(0, count - 1)], buffer.at[pl.ds(0, count - 1)], sem
        )

    def forward(level, toward_low):
        span, count, group = spans[level], counts[level], groups[level]
        seat = seats[level]
        target = picked[:, starts[level]:starts[level] + span] - toward_low[:, :span]
        left[level][:, :span] = target
        left[level][:, seat:seat + span] = -toward_low[:, span:]
        terms = dot(left[level][...], split_rows[level])
        out, into = scatter_out[level], scatter_in[level]
        for d in range(count):
            out[d, :, :span] = terms[:, d * span:(d + 1) * span]
        mine = place(group)

        def send(k, carry):
            d = (mine + k) % count
            pltpu.make_async_remote_copy(
                src_ref=out.at[d], dst_ref=into.at[mine],
                send_sem=s_send.at[level], recv_sem=s_recv.at[level],
                device_id=coords(group, d), device_id_type=MESH,
            ).start()
            return carry

        lax.fori_loop(1, count, send, 0)
        into[mine] = out[mine]

    def forward_end(level):
        into = scatter_in[level]
        all_slots(into, s_recv.at[level], counts[level]).wait()
        return jnp.sum(into[...], axis=0)[:, :spans[level]]

    def backward(level, gap):
        span, count, group = spans[level], counts[level], groups[level]
        into = gather_in[level]
        own = stage[level]
        mine = place(group)
        own[:, :span] = gap

        def send(k, carry):
            d = (mine + k) % count
            pltpu.make_async_remote_copy(
                src_ref=own, dst_ref=into.at[mine],
                send_sem=g_send.at[level], recv_sem=g_recv.at[level],
                device_id=coords(group, d), device_id_type=MESH,
            ).start()
            return carry

        lax.fori_loop(1, count, send, 0)
        into[mine] = own[...]

    def backward_end(level):
        span, count, seat = spans[level], counts[level], seats[level]
        into = gather_in[level]
        all_slots(into, g_recv.at[level], count).wait()
        full = whole[level]
        for d in range(count):
            full[:, d * span:(d + 1) * span] = into[d, :, :span]
        value = full[...]
        pair = pairs[level]
        solved = dot_back(value, split_rows[level])
        back = solved[:, :span]
        pair[:, :span] = back
        pair[:, span:] = solved[:, seat:seat + span]
        return back, pair[...]

    to_first, to_second, to_top = split_links
    forward(0, dot_back(leaf_solved, to_first))
    second_low = dot_back(leaf_solved, to_second)
    top_low = dot_back(leaf_solved, to_top)
    first_own = forward_end(0)
    forward(1, second_low + dot(first_own, split_fs))
    top_low = top_low + dot(first_own, split_ft)
    settle(2)
    second_own = forward_end(1)
    forward(2, top_low + dot(second_own, split_st))
    top_own = forward_end(2)
    backward(2, top_own)
    top_back, top_pair = backward_end(2)
    backward(1, second_own - dot_back(top_pair, split_st))
    first_gap = first_own - dot_back(top_pair, split_ft)
    leaf_gap = leaf_solved - dot(top_pair, to_top)
    second_back, second_pair = backward_end(1)
    backward(0, first_gap - dot_back(second_pair, split_fs))
    leaf_gap = leaf_gap - dot(second_pair, to_second)
    first_back, first_pair = backward_end(0)
    leaf_back = dot_back(leaf_gap - dot(first_pair, to_first), split_leaf)
    ordered[:, :leaf] = leaf_back
    ordered[:, starts[0]:starts[1]] = first_back
    ordered[:, starts[1]:starts[2]] = second_back
    ordered[:, starts[2]:] = top_back

    cells_back = None
    for r in range(rhs):
        term = dot_exact(row_hot * ordered[r:r + 1, :], lane_hot(r), single_back)
        cells_back = term if cells_back is None else cells_back + term
    rim[0, 0, 0:side] = cells_back.reshape(side, pad_y, LANES)

    rim_copies = []
    for n, step in enumerate(RIMS):
        dx, dy, dz = step
        source = rim.at[0, 0, pl.ds(0, 1 if dx else side)]
        landing = rim.at[dy, dz, pl.ds(side, 1) if dx else pl.ds(0, side)]
        copy = pltpu.make_async_remote_copy(
            src_ref=source, dst_ref=landing,
            send_sem=r_send.at[n], recv_sem=r_recv.at[n],
            device_id=toward(step, -1), device_id_type=MESH,
        )
        rim_copies.append(copy)

        @pl.when(valid(step, -1))
        def _():
            copy.start()

    for n, step in enumerate(RIMS):
        dx, dy, dz = step
        here = valid(step, 1)

        @pl.when(here)
        def _():
            rim_copies[n].wait_recv()

        @pl.when(jnp.logical_not(here))
        def _():
            if dx:
                rim[dy, dz, side] = jnp.zeros((pad_y, LANES), f32)
            else:
                rim[dy, dz, 0:side] = jnp.zeros((side, pad_y, LANES), f32)

    tall_rows = (side + 1) * pad_y
    grown = None
    for s in range(2):
        wide = dot_exact(rim[s, 0].reshape(tall_rows, LANES), mat_wide[0])
        wide = wide + dot_exact(rim[s, 1].reshape(tall_rows, LANES), mat_wide[1])
        high, low = halves(wide)
        term = single(mat_tall[s], high) + single(mat_tall[s], low)
        grown = term if grown is None else grown + term
    for r in range(rhs):
        slices = [
            grown[at * ny:(at + 1) * ny, r * nz:(r + 1) * nz] for at in range(side + 1)
        ]
        for x in range(nx):
            at, k = x // 4, x % 4
            if k == 0:
                out_ref[r, x] = slices[at]
            else:
                out_ref[r, x] = (1 - k / 4) * slices[at] + (k / 4) * slices[at + 1]

    for level in range(3):
        axis = shift_axis[level]

        @pl.when(me[axis] < peers[axis] - 1)
        def _():
            prev_copies[level].wait_send()

        all_slots(scatter_out[level], s_send.at[level], counts[level]).wait()
        all_slots(gather_in[level], g_send.at[level], counts[level]).wait()
    for n, step in enumerate(SHARES):
        @pl.when(valid(step, 1))
        def _():
            share_copies[n].wait_send()
    for n, step in enumerate(RIMS):
        @pl.when(valid(step, -1))
        def _():
            rim_copies[n].wait_send()


def per_device(peers, right_side, iterate, coefficient, ordering, leaf_inverse, leaf_first,
               leaf_second, leaf_top, first_inverse, first_second, first_top, second_inverse,
               second_top, top_inverse):
    rhs, nx, ny, nz = iterate.shape
    side = nx // 4
    slabs = side + 2
    pad_y = -(-(ny // 4) // 8) * 8
    pad_z = LANES // rhs // 4 if nz // 4 <= LANES // rhs // 4 else LANES // rhs
    mats = constants(rhs, ny, nz, slabs, pad_y, pad_z, side + 1)
    flip = lambda m: jnp.swapaxes(m, -1, -2)
    flat = lambda m: m.reshape(m.shape[-2:])
    single_rows = lambda m: m.reshape(m.shape[-2], 1, m.shape[-1])
    rows = [single_rows(first_inverse), single_rows(second_inverse), top_inverse]
    spans = [m.shape[0] for m in rows]
    widths = [m.shape[-1] for m in rows]
    counts = [w // s for w, s in zip(widths, spans)]
    seats = [-(-s // 16) * 16 for s in spans]
    leaf = leaf_inverse.shape[-1]
    cells = ordering.shape[-1]
    vmem = lambda *shape: pltpu.VMEM(shape, f32)
    split = lambda *shape: [pltpu.VMEM(shape, bf16)] * 2
    dma = lambda n: pltpu.SemaphoreType.DMA((n,))
    tile = (pad_y, LANES)
    sizes = {"peers": peers, "pad_y": pad_y, "pad_z": pad_z}
    operands = (
        right_side, iterate, coefficient, ordering.reshape(1, cells), single_rows(leaf_inverse),
        single_rows(flip(leaf_first)), single_rows(flip(leaf_second)), flat(flip(leaf_top)),
        single_rows(first_second), single_rows(first_top), single_rows(second_top), *rows,
        *[jnp.asarray(m, bf16) for m in mats],
    )
    in_vmem = pl.BlockSpec(memory_space=pltpu.VMEM)
    return pl.pallas_call(
        functools.partial(kernel, sizes),
        out_shape=jax.ShapeDtypeStruct(iterate.shape, f32),
        in_specs=jax.tree.map(lambda _: in_vmem, operands),
        out_specs=in_vmem,
        scratch_shapes=[
            split(leaf, leaf),
            [split(2 * s, leaf) for s in spans],
            split(spans[0], 2 * spans[1]),
            split(spans[0], 2 * spans[2]),
            split(spans[1], 2 * spans[2]),
            [split(2 * seat, w) for seat, w in zip(seats, widths)],
            [vmem(rhs, 2 * seat) for seat in seats],
            vmem(2 * slabs * ny, rhs * nz),
            vmem(3, 3, slabs, *tile),
            vmem(side, *tile),
            [vmem(side if step[0] == 0 else 1, *tile) for step in SHARES],
            [vmem(*m.shape) for m in rows],
            [vmem(n, rhs, LANES) for n in counts],
            [vmem(n, rhs, LANES) for n in counts],
            [vmem(n, rhs, LANES) for n in counts],
            [vmem(rhs, w) for w in widths],
            [vmem(rhs, 2 * s) for s in spans],
            vmem(rhs, cells),
            vmem(rhs, cells),
            vmem(2, 2, side + 1, *tile),
            [vmem(rhs, LANES) for _ in rows],
            dma(len(SHARES)), dma(len(SHARES)), dma(3), dma(3), dma(3), dma(3), dma(3), dma(3),
            dma(len(RIMS)), dma(len(RIMS)),
        ],
        compiler_params=pltpu.CompilerParams(has_side_effects=True),
    )(*operands)


def solution(mesh):
    peers = dict(mesh.shape)
    return jax.shard_map(
        functools.partial(per_device, peers),
        mesh=mesh,
        in_specs=(
            P(None, "gx", "gy", "gz"),
            P(None, "gx", "gy", "gz"),
            P("gx", "gy", "gz"),
            P("gx", "gy", "gz", None),
            P("gx", "gy", "gz", None, None),
            P("gx", "gy", "gz", None, None),
            P("gx", "gy", "gz", None, None),
            P("gx", "gy", "gz", None, None),
            P("gx", "gy", "gz", None),
            P("gx", "gy", "gz", None, None),
            P("gx", "gy", "gz", None, None),
            P("gx", ("gy", "gz"), None),
            P("gx", "gy", "gz", None, None),
            P(("gx", "gy", "gz"), None),
        ),
        out_specs=P(None, "gx", "gy", "gz"),
        check_vma=False,
    )
```

```python
import functools

import jax
import jax.numpy as jnp
import numpy as np
from jax import lax
from jax.experimental import pallas as pl
from jax.experimental.pallas import tpu as pltpu
from jax.sharding import PartitionSpec as P

AXES = ("gx", "gy", "gz")
LANES = 128
SIDES = (0, 1, -1)
MESH = pl.DeviceIdType.MESH
f32 = jnp.float32
bf16 = jnp.bfloat16

SHARES = [
    (i, j, k)
    for i in SIDES
    for j in SIDES
    for k in SIDES
    if (i, j, k) != (0, 0, 0) and (i, j, k).count(-1) <= 1
]
RIMS = [(i, j, k) for i in (0, 1) for j in (0, 1) for k in (0, 1) if (i, j, k) != (0, 0, 0)]


def weight(k):
    return max(0, 4 - abs(k)) / 16.0


def weight_beside(k):
    return weight(k - 1) + weight(k + 1)


def single(a, b):
    return jnp.dot(a, b, preferred_element_type=f32)


def single_back(a, b):
    return lax.dot_general(a, b, (((1,), (1,)), ((), ())), preferred_element_type=f32)


def halves(x):
    high = x.astype(bf16)
    return high, (x - high.astype(f32)).astype(bf16)


def stacked(x):
    high = x.astype(bf16).astype(f32)
    return jnp.concatenate([high, x - high], axis=0).astype(bf16)


def dot_exact(a, b, product=single):
    high, low = halves(a)
    return product(high, b) + product(low, b)


def dot(a, b, product=single):
    count = a.shape[0]
    both = product(stacked(a), b[0][...])
    return both[:count] + both[count:] + product(a.astype(bf16), b[1][...])


def dot_back(a, b):
    return dot(a, b, single_back)


def coarse_at(side, row, count):
    if side == 0:
        return row if row < count else None
    if side == 1:
        return count if row == 0 else None
    return -1 if row == count - 1 else None


def restriction(fine, pad, stencil):
    count = fine // 4
    out = np.zeros((3, pad, fine), np.float32)
    for s, side in enumerate(SIDES):
        for row in range(pad):
            at = coarse_at(side, row, count)
            if at is not None:
                for y in range(fine):
                    out[s, row, y] = stencil(y - 4 * at)
    return out


def at_first(table):
    table = table.copy()
    table[0, 0, 0] -= weight(-1)
    return table


def interpolation(fine, pad):
    count = fine // 4
    out = np.zeros((2, fine, pad), np.float32)
    for y in range(fine):
        for at in (y // 4, y // 4 + 1):
            value = 1.0 - abs(y - 4 * at) / 4.0
            if at < count:
                out[0, y, at] = value
            else:
                out[1, y, 0] = value
    return out


def constants(rhs, ny, nz, slabs, pad_y, pad_z, rims):
    plain = restriction(ny, pad_y, weight)
    beside = restriction(ny, pad_y, weight_beside)
    eye = np.eye(slabs, dtype=np.float32)
    rows = np.stack([
        np.concatenate(
            [np.concatenate([np.kron(eye, plain[s]), np.kron(eye, b[s])], 1) for s in range(3)], 0
        )
        for b in (at_first(beside), beside)
    ])

    def over_lanes(table):
        out = np.zeros((3, rhs * nz, LANES), np.float32)
        for s in range(3):
            for r in range(rhs):
                out[s, r * nz:(r + 1) * nz, r * pad_z:(r + 1) * pad_z] = table[s].T
        return np.concatenate(list(out), 1)

    lanes = over_lanes(restriction(nz, pad_z, weight))
    table = restriction(nz, pad_z, weight_beside)
    lanes_beside = np.stack([over_lanes(at_first(table)), over_lanes(table)])
    grow = interpolation(nz, pad_z)
    wide = np.zeros((2, LANES, rhs * nz), np.float32)
    for s in range(2):
        for r in range(rhs):
            wide[s, r * pad_z:(r + 1) * pad_z, r * nz:(r + 1) * nz] = grow[s].T
    eye = np.eye(rims, dtype=np.float32)
    tall_of = interpolation(ny, pad_y)
    tall = np.stack([np.kron(eye, tall_of[s]) for s in range(2)])
    return rows, lanes, lanes_beside, wide, tall


def kernel(
    sizes,
    right_ref, u_ref, coef_ref, order_ref, leaf_raw, leaf_first_raw, leaf_second_raw,
    leaf_top_ref, fs_raw, ft_raw, st_raw, rows_first, rows_second, rows_top,
    mat_rows, mat_lanes, mat_beside, mat_wide, mat_tall,
    out_ref,
    split_leaf, split_links, split_fs, split_ft, split_st, split_rows, left,
    packed, shares, total, share_in, prev, scatter_out, scatter_in, gather_in, whole, pairs,
    picked, ordered, rim, stage,
    share_send, share_recv, prev_send, prev_recv, s_send, s_recv, g_send, g_recv, r_send, r_recv,
):
    rhs, nx, ny, nz = u_ref.shape
    side = nx // 4
    side_y, side_z = ny // 4, nz // 4
    slabs = side + 2
    pad_y, pad_z = sizes["pad_y"], sizes["pad_z"]
    me = {a: lax.axis_index(a) for a in AXES}
    peers = sizes["peers"]
    rows_refs = (rows_first, rows_second, rows_top)
    groups = (("gz",), ("gy", "gz"), AXES)
    shift_axis = ("gz", "gy", "gx")
    counts = [int(np.prod([peers[a] for a in g])) for g in groups]

    def place(group):
        at = 0
        for a in group:
            at = at * peers[a] + me[a]
        return at

    def coords(group, at):
        found = {}
        for a in reversed(group):
            found[a] = at % peers[a]
            at = at // peers[a]
        return {a: found[a] if a in found else me[a] for a in AXES}

    barrier = pltpu.get_barrier_semaphore()
    everyone, myself = counts[2], place(AXES)

    def greet(k, carry):
        pl.semaphore_signal(
            barrier, inc=1, device_id=coords(AXES, (myself + k) % everyone), device_id_type=MESH
        )
        return carry

    lax.fori_loop(1, everyone, greet, 0)

    prev_copies = []
    for level in range(3):
        axis = shift_axis[level]
        target = dict(me)
        target[axis] = (me[axis] + 1) % peers[axis]
        copy = pltpu.make_async_remote_copy(
            src_ref=rows_refs[level], dst_ref=prev[level],
            send_sem=prev_send.at[level], recv_sem=prev_recv.at[level],
            device_id=target, device_id_type=MESH,
        )
        prev_copies.append(copy)

        @pl.when(me[axis] == 0)
        def _():
            prev[level][...] = jnp.zeros(prev[level].shape, f32)

    half = slabs * ny
    for r in range(rhs):
        acc_p = {}
        acc_u = {}

        def add(acc, at, factor, value):
            term = factor * value
            acc[at] = acc[at] + term if at in acc else term

        for x in range(nx):
            u = u_ref[r, x]
            q = right_ref[r, x] - (6.0 + coef_ref[x]) * u
            for at in range(-1, side + 1):
                k = x - 4 * at
                if weight(k):
                    add(acc_p, at, weight(k), q)
                    add(acc_u, at, weight(k), u)
                if at == 0 and x == 0:
                    below = jnp.where(me["gx"] > 0, weight(-1), 0.0)
                    add(acc_p, at, weight(1) + below, u)
                elif weight_beside(k):
                    add(acc_p, at, weight_beside(k), u)
        for at in range(-1, side + 1):
            rows = slice((at + 1) * ny, (at + 2) * ny)
            packed[rows, r * nz:(r + 1) * nz] = acc_p[at]
            rows = slice(half + (at + 1) * ny, half + (at + 2) * ny)
            packed[rows, r * nz:(r + 1) * nz] = acc_u.get(at, jnp.zeros((ny, nz), f32))
    both = packed[...]
    at_y, at_z = jnp.minimum(me["gy"], 1), jnp.minimum(me["gz"], 1)
    high, low = halves(both)
    a = single(mat_rows[at_y], high) + single(mat_rows[at_y], low)
    b = single(mat_rows[1, :, :half], high[half:]) + single(mat_rows[1, :, :half], low[half:])
    c = dot_exact(a, mat_lanes[...]) + dot_exact(b, mat_beside[at_z])
    for s in range(3):
        for t in range(3):
            part = c[s * slabs * pad_y:(s + 1) * slabs * pad_y, t * LANES:(t + 1) * LANES]
            shares[s, t] = part.reshape(slabs, pad_y, LANES)

    def valid(step, sign):
        ok = None
        for a, d in zip(AXES, step):
            if d:
                at = me[a] + sign * d
                this = (at >= 0) & (at < peers[a])
                ok = this if ok is None else ok & this
        return ok

    def toward(step, sign):
        return {a: (me[a] + sign * d + peers[a]) % peers[a] for a, d in zip(AXES, step)}

    pl.semaphore_wait(barrier, everyone - 1)
    for level in range(2):
        @pl.when(me[shift_axis[level]] < peers[shift_axis[level]] - 1)
        def _():
            prev_copies[level].start()

    share_copies = []
    for n, step in enumerate(SHARES):
        dx, dy, dz = step
        cut = {0: pl.ds(1, side), 1: pl.ds(side + 1, 1), -1: pl.ds(0, 1)}[dx]
        copy = pltpu.make_async_remote_copy(
            src_ref=shares.at[SIDES.index(dy), SIDES.index(dz), cut],
            dst_ref=share_in[n],
            send_sem=share_send.at[n], recv_sem=share_recv.at[n],
            device_id=toward(step, 1), device_id_type=MESH,
        )
        share_copies.append(copy)

        @pl.when(valid(step, 1))
        def _():
            copy.start()

    @pl.when(me[shift_axis[2]] < peers[shift_axis[2]] - 1)
    def _():
        prev_copies[2].start()

    total[...] = shares[0, 0, 1:side + 1]

    def keep(where, value):
        where[0][...], where[1][...] = halves(value)

    def rows_of(raw):
        return raw[:, 0, :] if len(raw.shape) == 3 else raw[...]

    spans = [rows.shape[0] for rows in rows_refs]
    seats = [split_rows[level][0].shape[0] // 2 for level in range(3)]

    def keep_rows(level, at, value):
        high, low = halves(value)
        split_rows[level][0][at:at + spans[level], :] = high
        split_rows[level][1][at:at + spans[level], :] = low

    keep(split_leaf, rows_of(leaf_raw))
    for where, raw in zip(split_links, (leaf_first_raw, leaf_second_raw, leaf_top_ref)):
        keep(where, rows_of(raw))
    keep(split_fs, rows_of(fs_raw))
    keep(split_ft, rows_of(ft_raw))
    keep(split_st, rows_of(st_raw))
    for level in range(3):
        for part in split_rows[level]:
            part[...] = jnp.zeros(part.shape, bf16)
        left[level][...] = jnp.zeros(left[level].shape, f32)
        keep_rows(level, 0, rows_of(rows_refs[level]))

    def settle(level):
        axis = shift_axis[level]

        @pl.when(me[axis] > 0)
        def _():
            prev_copies[level].wait_recv()

        keep_rows(level, seats[level], rows_of(prev[level]))

    settle(0)
    settle(1)

    order = order_ref[...].astype(f32)
    first = jnp.floor((order + 0.5) / (side_y * side_z))
    rest = order - first * (side_y * side_z)
    second = jnp.floor((rest + 0.5) / side_z)
    third = rest - second * side_z
    cells = order.shape[1]
    spots = side * pad_y
    row_id = lax.broadcasted_iota(jnp.int32, (spots, cells), 0).astype(f32)
    row_hot = (row_id == first * pad_y + second).astype(f32)
    lane_id = lax.broadcasted_iota(jnp.int32, (LANES, cells), 0).astype(f32)

    def lane_hot(r):
        return (lane_id == third + r * pad_z).astype(f32).astype(bf16)

    for n, step in enumerate(SHARES):
        @pl.when(valid(step, -1))
        def _():
            share_copies[n].wait_recv()
            if step[0] == 0:
                total[...] += share_in[n][...]
            elif step[0] == 1:
                total[0] += share_in[n][0]
            else:
                total[side - 1] += share_in[n][0]

    coarse = total[...].reshape(spots, LANES)
    for r in range(rhs):
        spread = dot_exact(coarse, lane_hot(r))
        picked[r:r + 1, :] = jnp.sum(spread * row_hot, axis=0, keepdims=True)

    leaf = leaf_raw.shape[0]
    starts = [leaf, leaf + spans[0], leaf + spans[0] + spans[1]]
    leaf_solved = dot(picked[:, :leaf], split_leaf)

    def all_slots(buffer, sem, count):
        return pltpu.make_async_copy(
            buffer.at[pl.ds(0, count - 1)], buffer.at[pl.ds(0, count - 1)], sem
        )

    def forward(level, toward_low):
        span, count, group = spans[level], counts[level], groups[level]
        seat = seats[level]
        target = picked[:, starts[level]:starts[level] + span] - toward_low[:, :span]
        left[level][:, :span] = target
        left[level][:, seat:seat + span] = -toward_low[:, span:]
        terms = dot(left[level][...], split_rows[level])
        out, into = scatter_out[level], scatter_in[level]
        for d in range(count):
            out[d, :, :span] = terms[:, d * span:(d + 1) * span]
        mine = place(group)

        def send(k, carry):
            d = (mine + k) % count
            pltpu.make_async_remote_copy(
                src_ref=out.at[d], dst_ref=into.at[mine],
                send_sem=s_send.at[level], recv_sem=s_recv.at[level],
                device_id=coords(group, d), device_id_type=MESH,
            ).start()
            return carry

        lax.fori_loop(1, count, send, 0)
        into[mine] = out[mine]

    def forward_end(level):
        into = scatter_in[level]
        all_slots(into, s_recv.at[level], counts[level]).wait()
        return jnp.sum(into[...], axis=0)[:, :spans[level]]

    def backward(level, gap):
        span, count, group = spans[level], counts[level], groups[level]
        into = gather_in[level]
        own = stage[level]
        mine = place(group)
        own[:, :span] = gap

        def send(k, carry):
            d = (mine + k) % count
            pltpu.make_async_remote_copy(
                src_ref=own, dst_ref=into.at[mine],
                send_sem=g_send.at[level], recv_sem=g_recv.at[level],
                device_id=coords(group, d), device_id_type=MESH,
            ).start()
            return carry

        lax.fori_loop(1, count, send, 0)
        into[mine] = own[...]

    def backward_end(level):
        span, count, seat = spans[level], counts[level], seats[level]
        into = gather_in[level]
        all_slots(into, g_recv.at[level], count).wait()
        full = whole[level]
        for d in range(count):
            full[:, d * span:(d + 1) * span] = into[d, :, :span]
        value = full[...]
        pair = pairs[level]
        solved = dot_back(value, split_rows[level])
        back = solved[:, :span]
        pair[:, :span] = back
        pair[:, span:] = solved[:, seat:seat + span]
        return back, pair[...]

    to_first, to_second, to_top = split_links
    forward(0, dot_back(leaf_solved, to_first))
    second_low = dot_back(leaf_solved, to_second)
    top_low = dot_back(leaf_solved, to_top)
    first_own = forward_end(0)
    forward(1, second_low + dot(first_own, split_fs))
    top_low = top_low + dot(first_own, split_ft)
    settle(2)
    second_own = forward_end(1)
    forward(2, top_low + dot(second_own, split_st))
    top_own = forward_end(2)
    backward(2, top_own)
    top_back, top_pair = backward_end(2)
    backward(1, second_own - dot_back(top_pair, split_st))
    first_gap = first_own - dot_back(top_pair, split_ft)
    leaf_gap = leaf_solved - dot(top_pair, to_top)
    second_back, second_pair = backward_end(1)
    backward(0, first_gap - dot_back(second_pair, split_fs))
    leaf_gap = leaf_gap - dot(second_pair, to_second)
    first_back, first_pair = backward_end(0)
    leaf_back = dot_back(leaf_gap - dot(first_pair, to_first), split_leaf)
    ordered[:, :leaf] = leaf_back
    ordered[:, starts[0]:starts[1]] = first_back
    ordered[:, starts[1]:starts[2]] = second_back
    ordered[:, starts[2]:] = top_back

    cells_back = None
    for r in range(rhs):
        term = dot_exact(row_hot * ordered[r:r + 1, :], lane_hot(r), single_back)
        cells_back = term if cells_back is None else cells_back + term
    rim[0, 0, 0:side] = cells_back.reshape(side, pad_y, LANES)

    rim_copies = []
    for n, step in enumerate(RIMS):
        dx, dy, dz = step
        source = rim.at[0, 0, pl.ds(0, 1 if dx else side)]
        landing = rim.at[dy, dz, pl.ds(side, 1) if dx else pl.ds(0, side)]
        copy = pltpu.make_async_remote_copy(
            src_ref=source, dst_ref=landing,
            send_sem=r_send.at[n], recv_sem=r_recv.at[n],
            device_id=toward(step, -1), device_id_type=MESH,
        )
        rim_copies.append(copy)

        @pl.when(valid(step, -1))
        def _():
            copy.start()

    for n, step in enumerate(RIMS):
        dx, dy, dz = step
        here = valid(step, 1)

        @pl.when(here)
        def _():
            rim_copies[n].wait_recv()

        @pl.when(jnp.logical_not(here))
        def _():
            if dx:
                rim[dy, dz, side] = jnp.zeros((pad_y, LANES), f32)
            else:
                rim[dy, dz, 0:side] = jnp.zeros((side, pad_y, LANES), f32)

    tall_rows = (side + 1) * pad_y
    grown = None
    for s in range(2):
        wide = dot_exact(rim[s, 0].reshape(tall_rows, LANES), mat_wide[0])
        wide = wide + dot_exact(rim[s, 1].reshape(tall_rows, LANES), mat_wide[1])
        high, low = halves(wide)
        term = single(mat_tall[s], high) + single(mat_tall[s], low)
        grown = term if grown is None else grown + term
    out_ref[...] = grown

    for level in range(3):
        axis = shift_axis[level]

        @pl.when(me[axis] < peers[axis] - 1)
        def _():
            prev_copies[level].wait_send()

        all_slots(scatter_out[level], s_send.at[level], counts[level]).wait()
        all_slots(gather_in[level], g_send.at[level], counts[level]).wait()
    for n, step in enumerate(SHARES):
        @pl.when(valid(step, 1))
        def _():
            share_copies[n].wait_send()
    for n, step in enumerate(RIMS):
        @pl.when(valid(step, -1))
        def _():
            rim_copies[n].wait_send()


def spread_kernel(grown_ref, out_ref):
    rhs, nx, ny, nz = out_ref.shape
    side = nx // 4
    for r in range(rhs):
        slices = [
            grown_ref[at * ny:(at + 1) * ny, r * nz:(r + 1) * nz] for at in range(side + 1)
        ]
        for x in range(nx):
            at, k = x // 4, x % 4
            if k == 0:
                out_ref[r, x] = slices[at]
            else:
                out_ref[r, x] = (1 - k / 4) * slices[at] + (k / 4) * slices[at + 1]


def per_device(peers, right_side, iterate, coefficient, ordering, leaf_inverse, leaf_first,
               leaf_second, leaf_top, first_inverse, first_second, first_top, second_inverse,
               second_top, top_inverse):
    rhs, nx, ny, nz = iterate.shape
    side = nx // 4
    slabs = side + 2
    pad_y = -(-(ny // 4) // 8) * 8
    pad_z = LANES // rhs // 4 if nz // 4 <= LANES // rhs // 4 else LANES // rhs
    mats = constants(rhs, ny, nz, slabs, pad_y, pad_z, side + 1)
    flip = lambda m: jnp.swapaxes(m, -1, -2)
    flat = lambda m: m.reshape(m.shape[-2:])
    single_rows = lambda m: m.reshape(m.shape[-2], 1, m.shape[-1])
    rows = [single_rows(first_inverse), single_rows(second_inverse), top_inverse]
    spans = [m.shape[0] for m in rows]
    widths = [m.shape[-1] for m in rows]
    counts = [w // s for w, s in zip(widths, spans)]
    seats = [-(-s // 16) * 16 for s in spans]
    leaf = leaf_inverse.shape[-1]
    cells = ordering.shape[-1]
    vmem = lambda *shape: pltpu.VMEM(shape, f32)
    split = lambda *shape: [pltpu.VMEM(shape, bf16)] * 2
    dma = lambda n: pltpu.SemaphoreType.DMA((n,))
    tile = (pad_y, LANES)
    sizes = {"peers": peers, "pad_y": pad_y, "pad_z": pad_z}
    operands = (
        right_side, iterate, coefficient, ordering.reshape(1, cells), single_rows(leaf_inverse),
        single_rows(flip(leaf_first)), single_rows(flip(leaf_second)), flat(flip(leaf_top)),
        single_rows(first_second), single_rows(first_top), single_rows(second_top), *rows,
        *[jnp.asarray(m, bf16) for m in mats],
    )
    in_vmem = pl.BlockSpec(memory_space=pltpu.VMEM)
    grown = pl.pallas_call(
        functools.partial(kernel, sizes),
        out_shape=jax.ShapeDtypeStruct(((side + 1) * ny, rhs * nz), f32),
        in_specs=jax.tree.map(lambda _: in_vmem, operands),
        out_specs=in_vmem,
        scratch_shapes=[
            split(leaf, leaf),
            [split(2 * s, leaf) for s in spans],
            split(spans[0], 2 * spans[1]),
            split(spans[0], 2 * spans[2]),
            split(spans[1], 2 * spans[2]),
            [split(2 * seat, w) for seat, w in zip(seats, widths)],
            [vmem(rhs, 2 * seat) for seat in seats],
            vmem(2 * slabs * ny, rhs * nz),
            vmem(3, 3, slabs, *tile),
            vmem(side, *tile),
            [vmem(side if step[0] == 0 else 1, *tile) for step in SHARES],
            [vmem(*m.shape) for m in rows],
            [vmem(n, rhs, LANES) for n in counts],
            [vmem(n, rhs, LANES) for n in counts],
            [vmem(n, rhs, LANES) for n in counts],
            [vmem(rhs, w) for w in widths],
            [vmem(rhs, 2 * s) for s in spans],
            vmem(rhs, cells),
            vmem(rhs, cells),
            vmem(2, 2, side + 1, *tile),
            [vmem(rhs, LANES) for _ in rows],
            dma(len(SHARES)), dma(len(SHARES)), dma(3), dma(3), dma(3), dma(3), dma(3), dma(3),
            dma(len(RIMS)), dma(len(RIMS)),
        ],
        compiler_params=pltpu.CompilerParams(has_side_effects=True, collective_id=0),
    )(*operands)
    return pl.pallas_call(
        spread_kernel,
        out_shape=jax.ShapeDtypeStruct(iterate.shape, f32),
        in_specs=[in_vmem],
        out_specs=in_vmem,
    )(grown)


def solution(mesh):
    peers = dict(mesh.shape)
    return jax.shard_map(
        functools.partial(per_device, peers),
        mesh=mesh,
        in_specs=(
            P(None, "gx", "gy", "gz"),
            P(None, "gx", "gy", "gz"),
            P("gx", "gy", "gz"),
            P("gx", "gy", "gz", None),
            P("gx", "gy", "gz", None, None),
            P("gx", "gy", "gz", None, None),
            P("gx", "gy", "gz", None, None),
            P("gx", "gy", "gz", None, None),
            P("gx", "gy", "gz", None),
            P("gx", "gy", "gz", None, None),
            P("gx", "gy", "gz", None, None),
            P("gx", ("gy", "gz"), None),
            P("gx", "gy", "gz", None, None),
            P(("gx", "gy", "gz"), None),
        ),
        out_specs=P(None, "gx", "gy", "gz"),
        check_vma=False,
    )
```
